32 devices in a mesh: section: 4 (over z), batch: 2 (over x), tile: 4 (over y, core).
Axes of the slice: x: 2, y: 2, z: 4, core: 2. Of those that a mesh axis runs over, the one named last changes fastest.
Arguments:
- latents: bfloat16 [8, 4, 32, 1280], P('batch', 'tile'), parts along dimension 0, may hold values from -6 to 6
- prompt_tokens: bfloat16 [8, 77, 2048], P('batch'), parts along dimension 0, may hold values from -6 to 6
- fresh_noise: bfloat16 [1, 8, 4, 32, 1280], P(None, 'batch', 'tile'), parts along dimension 1, may hold values from -6 to 6
- timesteps: int32 [2], replicated, may hold values from 600 to 999
- entry_order: int32 [8], P('batch'), parts along dimension 0, may hold values from 0 to 3, each once
- timestep_weight: bfloat16 [4, 320, 1280], P('section'), may hold values from -0.3125 to 0.3125
- conv_kernel: float32 [4, 9, 1280], P('section'), may hold values from -1 to 1
- norm_gain: float32 [4, 1280], P('section'), may hold values from 0.25 to 1.75
- layer_norm_bias: float32 [4, 1280], P('section'), may hold values from -1.5 to 1.5
- qkv_weight: bfloat16 [4, 1280, 3, 1280], P('section', None, None, 'tile'), may hold values from -0.15625 to 0.15625
- prompt_weight: bfloat16 [4, 2048, 2, 1280], P('section', None, None, 'tile'), may hold values from -0.125 to 0.125
- out_weight: bfloat16 [4, 1280, 1280], P('section', 'tile'), may hold values from -0.15625 to 0.15625
Outputs:
- samples: bfloat16 [8, 4, 32, 1280], P('batch', 'tile', None, 'section'), parts along dimension 0
The draws below stay inside these ranges and needn't reach their ends.
There are 2 independent parts, one for each index of `batch`. The reference program is written for one: setup_inputs(seed, part) draws one part's arguments, and reference() takes and returns one part's arrays. A program takes and returns all parts, laid end to end along the dimension named above; an argument that names none is the same for every part. Nothing has to cross between parts.
All inputs are finite; a program needn't handle non-finite values.
Results may differ from the reference program's by a relative error of at most 0.019.
Values may be sent and summed in bfloat16 or wider, within the bound.
A program may use at most 64 MiB of HBM per device.

```python
import math
import jax
import jax.numpy as jnp
from jax import lax

WIDTH = 1280
HEADS = 20
TEXT_WIDTH = 2048
FREQS = 320
TEXT_TOKENS = 77
COLS = 32
ROWS = 4
MICRO = 4
STEPS = 2
N_SECTION = 4


def levels(stream_key, shape, split, low, largest):
    level = 1.0
    for axis_at, blocks in split:
        steps = jax.random.uniform(jax.random.fold_in(jax.random.fold_in(stream_key, 6), axis_at), (blocks,), jnp.float32, low / len(split), largest / len(split))
        level = level * jnp.repeat(jnp.exp(steps), shape[axis_at] // blocks).reshape((-1,) + (1,) * (len(shape) - 1 - axis_at))
    return level


def noise(key, shape, scale, most, shards=(), kind=jnp.bfloat16):
    drawn = jax.random.normal(key, shape, jnp.float32) * scale
    if len(shards) > 0:
        drawn = levels(key, shape, shards, -0.22, 0.18) * drawn
    return jnp.clip(drawn, min=-most, max=most).astype(kind)


def setup_inputs(seed: int = 0, part: int = 0) -> dict:
    seeds = jax.random.split(jax.random.key(seed), 13)
    own_keys = jax.random.split(jax.random.fold_in(seeds[12], part), 13)
    latents = noise(own_keys[0], (MICRO, ROWS, COLS, WIDTH), 1.0, 6.0, ((1, 4),))
    prompt_tokens = noise(own_keys[1], (MICRO, TEXT_TOKENS, TEXT_WIDTH), 1.0, 6.0)
    fresh_noise = noise(own_keys[2], (STEPS - 1, MICRO, ROWS, COLS, WIDTH), 1.0, 6.0, ((2, 4),))
    timesteps = jax.random.randint(seeds[3], (STEPS,), 600, 1000).astype(jnp.int32)
    entry_order = jax.random.permutation(own_keys[4], MICRO).astype(jnp.int32)
    timestep_weight = noise(seeds[5], (N_SECTION, FREQS, WIDTH), FREQS ** -0.5, 0.3125, ((0, 4),))
    conv_kernel = noise(seeds[6], (N_SECTION, 9, WIDTH), 0.2, 1.0, ((0, 4),), jnp.float32)
    norm_gain = jnp.clip(1.0 + 0.15 * jax.random.normal(seeds[7], (N_SECTION, WIDTH), jnp.float32), 0.25, 1.75)
    layer_norm_bias = noise(seeds[8], (N_SECTION, WIDTH), 0.3, 1.5, ((0, 4),), jnp.float32)
    qkv_weight = noise(seeds[9], (N_SECTION, WIDTH, 3, WIDTH), WIDTH ** -0.5, 0.15625, ((0, 4), (3, 4)))
    prompt_weight = noise(seeds[10], (N_SECTION, TEXT_WIDTH, 2, WIDTH), TEXT_WIDTH ** -0.5, 0.125, ((0, 4), (3, 4)))
    out_weight = noise(seeds[11], (N_SECTION, WIDTH, WIDTH), WIDTH ** -0.5, 0.15625, ((0, 4), (1, 4)))
    return dict(latents=latents, prompt_tokens=prompt_tokens, fresh_noise=fresh_noise, timesteps=timesteps, entry_order=entry_order, timestep_weight=timestep_weight, conv_kernel=conv_kernel, norm_gain=norm_gain, layer_norm_bias=layer_norm_bias, qkv_weight=qkv_weight, prompt_weight=prompt_weight, out_weight=out_weight)


def noise_plan():
    positions = jnp.arange(1000, dtype=jnp.float32)
    low_root = math.sqrt(0.00085)
    high_root = math.sqrt(0.012)
    roots = low_root + (high_root - low_root) * positions / 999.0
    return jnp.exp(jnp.cumsum(jnp.log(1.0 - roots * roots)))

def time_features(timesteps, half_count):
    exponents = jnp.arange(half_count, dtype=jnp.float32) / half_count
    freq_row = jnp.exp(-math.log(10000.0) * exponents)
    angles = timesteps.astype(jnp.float32)[:, None] * freq_row[None, :]
    return jnp.concatenate([jnp.cos(angles), jnp.sin(angles)], axis=1).astype(jnp.bfloat16)

def pick_scalar(alpha_table, position):
    hits = jnp.arange(alpha_table.shape[0], dtype=jnp.int32) == position
    return jnp.sum(jnp.where(hits, alpha_table, jnp.zeros_like(alpha_table)))

def mix_positions(rimmed, kernel_body):
    row_total = rimmed.shape[0] - 2
    col_total = rimmed.shape[1]
    framed = jnp.pad(rimmed.astype(jnp.float32), ((0, 0), (1, 1), (0, 0)))
    mixed = rimmed[1:-1].astype(jnp.float32)
    for offset_row in range(3):
        for offset_col in range(3):
            mixed = mixed + kernel_body[3 * offset_row + offset_col] * framed[offset_row:offset_row + row_total, offset_col:offset_col + col_total]
    return mixed

def layer_norm(values_in, scale_row, shift_row):
    centre = lax.optimization_barrier(jnp.mean(values_in, axis=-1, keepdims=True))
    spread = lax.optimization_barrier(jnp.mean(jnp.square(values_in - centre), axis=-1, keepdims=True))
    return (values_in - centre) * lax.rsqrt(spread + 1e-05) * scale_row + shift_row

def attention(queries, keys_all, values_all, head_count):
    query_count = queries.shape[0]
    key_count = keys_all.shape[0]
    head_width = queries.shape[1] // head_count
    query_heads = queries.astype(jnp.float32).reshape(query_count, head_count, head_width)
    key_heads = keys_all.astype(jnp.float32).reshape(key_count, head_count, head_width)
    value_heads = values_all.astype(jnp.float32).reshape(key_count, head_count, head_width)
    scores = jnp.einsum('qhd,khd->hqk', query_heads, key_heads) / math.sqrt(head_width)
    powers = jnp.exp(scores)
    soft_weights = (powers / lax.optimization_barrier(jnp.sum(powers, axis=-1, keepdims=True))).astype(jnp.bfloat16)
    attended = jnp.einsum('hqk,khd->qhd', soft_weights.astype(jnp.float32), value_heads)
    return attended.reshape(query_count, head_count * head_width).astype(jnp.bfloat16)

def run_section(current, temb_row, kernel_body, scale_row, shift_row, qkv_mat, prompt_mat, out_mat, prompt_row):
    rows_all, cols_all, width_all = current.shape
    lifted = (current.astype(jnp.float32) + temb_row).astype(jnp.bfloat16)
    rimmed = jnp.pad(lifted, ((1, 1), (0, 0), (0, 0)))
    mixed = mix_positions(rimmed, kernel_body).reshape(rows_all * cols_all, width_all)
    normed = layer_norm(mixed, scale_row, shift_row).astype(jnp.bfloat16)
    projected = jnp.einsum('tc,cjd->tjd', normed.astype(jnp.float32), qkv_mat.astype(jnp.float32)).astype(jnp.bfloat16)
    prompt_proj = jnp.einsum('tc,cjd->tjd', prompt_row.astype(jnp.float32), prompt_mat.astype(jnp.float32)).astype(jnp.bfloat16)
    keys_all = jnp.concatenate([projected[:, 1], prompt_proj[:, 0]], axis=0)
    values_all = jnp.concatenate([projected[:, 2], prompt_proj[:, 1]], axis=0)
    attended = attention(projected[:, 0], keys_all, values_all, HEADS)
    update = jnp.dot(attended, out_mat, preferred_element_type=jnp.float32)
    return (mixed + update).astype(jnp.bfloat16).reshape(rows_all, cols_all, width_all)

def reference(latents, prompt_tokens, fresh_noise, timesteps, entry_order, timestep_weight, conv_kernel, norm_gain, layer_norm_bias, qkv_weight, prompt_weight, out_weight):
    alpha_table = noise_plan()
    feature_rows = time_features(timesteps, timestep_weight.shape[1] // 2)
    timestep_embedding_all = jnp.einsum('zm,rmk->rzk', feature_rows.astype(jnp.float32), timestep_weight.astype(jnp.float32))
    results = jnp.zeros_like(latents)
    for slot_index in range(MICRO):
        latent_id = entry_order[slot_index].astype(jnp.int32)
        current = lax.dynamic_index_in_dim(latents, latent_id, 0, False)
        prompt_row = lax.dynamic_index_in_dim(prompt_tokens, latent_id, 0, False)
        for chain_level in range(STEPS):
            if chain_level > 0:
                alpha_bar = pick_scalar(alpha_table, timesteps[chain_level])
                current = (jnp.sqrt(alpha_bar) * current.astype(jnp.float32) + jnp.sqrt(1.0 - alpha_bar) * fresh_noise[chain_level - 1, slot_index].astype(jnp.float32)).astype(jnp.bfloat16)

            def section_step(state_now, section_inputs):
                temb_row, kernel_body, scale_row, shift_row, qkv_mat, prompt_mat, out_mat = section_inputs
                return (run_section(state_now, temb_row, kernel_body, scale_row, shift_row, qkv_mat, prompt_mat, out_mat, prompt_row), None)
            section_inputs = (timestep_embedding_all[:, chain_level], conv_kernel, norm_gain, layer_norm_bias, qkv_weight, prompt_weight, out_weight)
            scanned = lax.scan(section_step, current, section_inputs)
            current = scanned[0]
        results = results.at[latent_id].set(current)
    return results
```

```python
import functools
import math

import jax
import jax.numpy as jnp
from jax import lax
from jax.experimental import pallas as pl
from jax.experimental.pallas import tpu as pltpu
from jax.sharding import PartitionSpec as P

HEADS = 20
LANES = 128
MESH = pl.DeviceIdType.MESH


def noise_plan():
    positions = jnp.arange(1000, dtype=jnp.float32)
    low_root = math.sqrt(0.00085)
    high_root = math.sqrt(0.012)
    roots = low_root + (high_root - low_root) * positions / 999.0
    return jnp.exp(jnp.cumsum(jnp.log(1.0 - roots * roots)))


def time_features(timesteps, half_count):
    exponents = jnp.arange(half_count, dtype=jnp.float32) / half_count
    freq_row = jnp.exp(-math.log(10000.0) * exponents)
    angles = timesteps.astype(jnp.float32)[:, None] * freq_row[None, :]
    return jnp.concatenate([jnp.cos(angles), jnp.sin(angles)], axis=1).astype(jnp.bfloat16)


def pick_scalar(alpha_table, position):
    hits = jnp.arange(alpha_table.shape[0], dtype=jnp.int32) == position
    return jnp.sum(jnp.where(hits, alpha_table, jnp.zeros_like(alpha_table)))


def chain_kernel(
    dims,
    coef_ref,
    x0_ref,
    noise_ref,
    temb_ref,
    conv_ref,
    gain_ref,
    bias_ref,
    qkv_ref,
    pkv_ref,
    outw_ref,
    out_ref,
    xin,
    xsend,
    psend,
    precv,
    mixed,
    mixed_own,
    normed,
    proj,
    osend,
    oland,
    x_recv,
    x_send,
    x_fwd,
    p_recv,
    p_send,
    o_recv,
    o_send,
):
    S, T, G, K, M, C, keys_prompt, local_heads, head_width = dims
    n, W = x0_ref.shape[1], x0_ref.shape[2]
    N = T * n
    Q = K * M
    J = T // G
    Hp = outw_ref.shape[0]
    Ws = out_ref.shape[2]
    s = lax.axis_index("section")
    t = lax.axis_index("tile")
    last = s == S - 1
    after = lax.rem(s + 1, S)
    partner = t + 1 - 2 * lax.rem(t, 2)

    barrier = pltpu.get_barrier_semaphore()
    for ds in range(S):
        for dt in range(T):
            if ds or dt:
                pl.semaphore_signal(
                    barrier,
                    inc=1,
                    device_id={"section": lax.rem(s + ds, S), "tile": lax.rem(t + dt, T)},
                    device_id_type=MESH,
                )
    pl.semaphore_wait(barrier, S * T - 1)

    def kin(tile, j):
        return lax.rem(tile + G * j, T)

    def x_copy(src, q, j):
        return pltpu.make_async_remote_copy(
            src_ref=src,
            dst_ref=xin.at[q, t],
            send_sem=x_send.at[q, j],
            recv_sem=x_recv.at[q, t],
            device_id={"section": after, "tile": kin(t, j)},
            device_id_type=MESH,
        )

    def x_relay(q, j):
        row = kin(t, j)
        return pltpu.make_async_remote_copy(
            src_ref=xin.at[q, row],
            dst_ref=xin.at[q, row],
            send_sem=x_fwd.at[q, j],
            recv_sem=x_recv.at[q, row],
            device_id={"section": s, "tile": partner},
            device_id_type=MESH,
        )

    def x_arrived(q, row):
        pltpu.make_async_copy(xin.at[q, row], xin.at[q, row], x_recv.at[q, row]).wait()

    def p_copy(q, d):
        other = lax.rem(t + d, T)
        return pltpu.make_async_remote_copy(
            src_ref=psend.at[q, other],
            dst_ref=precv.at[q, d - 1],
            send_sem=p_send.at[q, d - 1],
            recv_sem=p_recv.at[q, d - 1],
            device_id={"section": s, "tile": other},
            device_id_type=MESH,
        )

    def o_copy(i, d):
        other = lax.rem(s + d, S)
        return pltpu.make_async_remote_copy(
            src_ref=osend.at[i, other],
            dst_ref=oland.at[i],
            send_sem=o_send.at[i, d - 1],
            recv_sem=o_recv.at[i],
            device_id={"section": other, "tile": t},
            device_id_type=MESH,
        )

    @pl.when(last)
    def _():
        for i in range(M):
            for j in range(J):
                x_copy(x0_ref.at[i], i, j).start()

    column = lax.rem(lax.broadcasted_iota(jnp.int32, (N, LANES), 0), C)
    at_left = column == 0
    at_right = column == C - 1

    def compute(q, i, level):
        for j in range(J):
            x_arrived(q, kin(t, j))
            if G > 1:
                x_relay(q, j).start()
        if G > 1:
            for j in range(J):
                x_arrived(q, kin(partner, j))
        total = jnp.zeros((N, LANES), jnp.float32)
        for c in range(W // LANES):
            sl = slice(c * LANES, (c + 1) * LANES)
            x = xin[q, :, :, sl].reshape(N, LANES).astype(jnp.float32)
            x = (x + temb_ref[level, :, sl]).astype(jnp.bfloat16).astype(jnp.float32)
            left = jnp.where(at_left, 0.0, pltpu.roll(x, 1, 0))
            right = jnp.where(at_right, 0.0, pltpu.roll(x, N - 1, 0))
            taps = []
            for a in range(3):
                taps.append(
                    conv_ref[3 * a : 3 * a + 1, sl] * left
                    + conv_ref[3 * a + 1 : 3 * a + 2, sl] * x
                    + conv_ref[3 * a + 2 : 3 * a + 3, sl] * right
                )
            edge = jnp.zeros((C, LANES), jnp.float32)
            value = (
                x
                + jnp.concatenate([edge, taps[0][: N - C]], axis=0)
                + taps[1]
                + jnp.concatenate([taps[2][C:], edge], axis=0)
            )
            mixed[:, :, sl] = value.reshape(T, n, LANES)
            total = total + value
        centre = jnp.sum(total, axis=1, keepdims=True) / W
        total = jnp.zeros((N, LANES), jnp.float32)
        for c in range(W // LANES):
            sl = slice(c * LANES, (c + 1) * LANES)
            delta = mixed[:, :, sl].reshape(N, LANES) - centre
            total = total + delta * delta
        scale = lax.rsqrt(jnp.sum(total, axis=1, keepdims=True) / W + 1e-05)
        for c in range(W // LANES):
            sl = slice(c * LANES, (c + 1) * LANES)
            delta = mixed[:, :, sl].reshape(N, LANES) - centre
            normed[:, sl] = (delta * scale * gain_ref[:, sl] + bias_ref[:, sl]).astype(
                jnp.bfloat16
            )
        mixed_own[i] = mixed[t]
        proj[...] = jnp.dot(
            normed[...], qkv_ref[...], preferred_element_type=jnp.float32
        ).astype(jnp.bfloat16)
        per_block = LANES // head_width
        key_total = N + pkv_ref.shape[2]
        blocks = []
        for b in range(Hp // LANES):
            sl = slice(b * LANES, (b + 1) * LANES)
            heads_here = min(per_block, local_heads - b * per_block)
            query = proj[:, sl]
            keys = jnp.concatenate([proj[:, Hp + b * LANES : Hp + (b + 1) * LANES], pkv_ref[i, 0, :, sl]], axis=0)
            values = jnp.concatenate(
                [proj[:, 2 * Hp + b * LANES : 2 * Hp + (b + 1) * LANES], pkv_ref[i, 1, :, sl]], axis=0
            )
            lane = lax.broadcasted_iota(jnp.int32, (N, LANES), 1) // head_width
            zero = jnp.zeros_like(query)
            stacked = jnp.concatenate(
                [jnp.where(lane == h, query, zero) for h in range(heads_here)], axis=0
            )
            scores = lax.dot_general(
                stacked, keys, (((1,), (1,)), ((), ())), preferred_element_type=jnp.float32
            ) * (1.0 / math.sqrt(head_width))
            real = lax.broadcasted_iota(jnp.int32, scores.shape, 1) < N + keys_prompt
            powers = jnp.where(real, jnp.exp(scores), 0.0)
            soft = (powers * (1.0 / jnp.sum(powers, axis=1, keepdims=True))).astype(jnp.bfloat16)
            got = jnp.dot(soft, values, preferred_element_type=jnp.float32)
            merged = got[:N]
            for h in range(1, heads_here):
                merged = jnp.where(lane == h, got[h * N : (h + 1) * N], merged)
            blocks.append(merged.astype(jnp.bfloat16))
        attended = jnp.concatenate(blocks, axis=1)
        psend[q] = (
            jnp.dot(attended, outw_ref[...], preferred_element_type=jnp.float32)
            .astype(jnp.bfloat16)
            .reshape(T, n, W)
        )
        for d in range(1, T):
            p_copy(q, d).start()

    def finish(q, i, level):
        for d in range(1, T):
            p_copy(q, d).wait_recv()
        update = psend[q, t].astype(jnp.float32)
        for d in range(1, T):
            update = update + precv[q, d - 1].astype(jnp.float32)
        x = (mixed_own[i] + update).astype(jnp.bfloat16)
        final = jnp.logical_and(last, level == K - 1)

        @pl.when(jnp.logical_not(last))
        def _():
            xsend[q] = x
            for j in range(J):
                x_copy(xsend.at[q], q, j).start()

        if K > 1:

            @pl.when(jnp.logical_and(last, level < K - 1))
            def _():
                fresh = noise_ref[lax.rem(level, K - 1), i].astype(jnp.float32)
                later = lax.rem(level + 1, K)
                onward = lax.rem(q + M, Q)
                xsend[onward] = (
                    coef_ref[2 * later] * x.astype(jnp.float32) + coef_ref[2 * later + 1] * fresh
                ).astype(jnp.bfloat16)
                for j in range(J):
                    x_copy(xsend.at[onward], onward, j).start()

        @pl.when(final)
        def _():
            wide = x.astype(jnp.float32)
            for k in range(S):
                turned = wide if k == 0 else pltpu.roll(wide, W - k * Ws, 1)
                osend[i, k] = turned[:, :Ws].astype(jnp.bfloat16)
            for d in range(1, S):
                o_copy(i, d).start()

    def step(k, carry):
        level = k // (M + 1)
        i = lax.rem(k, M + 1)

        @pl.when(i < M)
        def _():
            here = lax.rem(i, M)
            compute(level * M + here, here, level)

        @pl.when(i > 0)
        def _():
            before = lax.rem(i + M - 1, M)
            finish(level * M + before, before, level)

        return carry

    lax.fori_loop(0, K * (M + 1), step, 0)

    def drain(q, carry):
        for j in range(J):
            x_copy(xsend.at[q], q, j).wait_send()
            if G > 1:
                x_relay(q, j).wait_send()
        for d in range(1, T):
            p_copy(q, d).wait_send()
        return carry

    lax.fori_loop(0, Q, drain, 0)

    @pl.when(last)
    def _():
        for i in range(M):
            out_ref[i] = osend[i, S - 1]
            for d in range(1, S):
                o_copy(i, d).wait_send()

    @pl.when(jnp.logical_not(last))
    def _():
        for i in range(M):
            pltpu.make_async_copy(oland.at[i], oland.at[i], o_recv.at[i]).wait()
            out_ref[i] = oland[i]


def per_device(
    latents,
    prompt_tokens,
    fresh_noise,
    timesteps,
    entry_order,
    timestep_weight,
    conv_kernel,
    norm_gain,
    layer_norm_bias,
    qkv_weight,
    prompt_weight,
    out_weight,
):
    S = lax.axis_size("section")
    T = lax.axis_size("tile")
    M, rows_here, C, W = latents.shape
    n = rows_here * C
    K = timesteps.shape[0]
    Q = K * M
    G = 2 if T % 2 == 0 else 1
    J = T // G
    local_heads = HEADS // T
    head_width = W // HEADS
    H = local_heads * head_width
    Hp = -(-H // LANES) * LANES
    text = prompt_tokens.shape[1]
    text_pad = -(-text // LANES) * LANES
    Ws = W // S

    alpha_table = noise_plan()
    alphas = jnp.stack([pick_scalar(alpha_table, timesteps[k]) for k in range(K)])
    coef = jnp.stack([jnp.sqrt(alphas), jnp.sqrt(1.0 - alphas)], axis=1).reshape(2 * K)
    feature_rows = time_features(timesteps, timestep_weight.shape[1] // 2)
    temb = jnp.dot(feature_rows, timestep_weight[0], preferred_element_type=jnp.float32)

    def ordered(array, index):
        return jnp.concatenate(
            [lax.dynamic_slice_in_dim(array, index[m], 1, 0) for m in range(M)], axis=0
        )

    x0 = ordered(latents, entry_order).reshape(M, n, W)
    noise = fresh_noise.reshape(fresh_noise.shape[0], M, n, W)
    tokens = prompt_tokens.reshape(M * text, prompt_tokens.shape[2])
    pkv = jnp.stack(
        [
            jnp.dot(tokens, prompt_weight[0, :, j], preferred_element_type=jnp.float32)
            .astype(jnp.bfloat16)
            .reshape(M, text, H)
            for j in range(2)
        ],
        axis=1,
    )
    pkv = jnp.pad(pkv, ((0, 0), (0, 0), (0, text_pad - text), (0, Hp - H)))
    pkv = ordered(pkv, entry_order)
    qkv = jnp.concatenate(
        [jnp.pad(qkv_weight[0, :, j], ((0, 0), (0, Hp - H))) for j in range(3)], axis=1
    )
    outw = jnp.pad(out_weight[0], ((0, Hp - H), (0, 0)))

    dims = (S, T, G, K, M, C, text, local_heads, head_width)
    vmem = pl.BlockSpec(memory_space=pltpu.VMEM)
    bf16, f32 = jnp.bfloat16, jnp.float32
    dma = pltpu.SemaphoreType.DMA
    results = pl.pallas_call(
        functools.partial(chain_kernel, dims),
        out_shape=jax.ShapeDtypeStruct((M, n, Ws), bf16),
        in_specs=[pl.BlockSpec(memory_space=pltpu.SMEM)] + [vmem] * 9,
        out_specs=vmem,
        scratch_shapes=[
            pltpu.VMEM((Q, T, n, W), bf16),
            pltpu.VMEM((Q, n, W), bf16),
            pltpu.VMEM((Q, T, n, W), bf16),
            pltpu.VMEM((Q, T - 1, n, W), bf16),
            pltpu.VMEM((T, n, W), f32),
            pltpu.VMEM((M, n, W), f32),
            pltpu.VMEM((T * n, W), bf16),
            pltpu.VMEM((T * n, 3 * Hp), bf16),
            pltpu.VMEM((M, S, n, Ws), bf16),
            pltpu.VMEM((M, n, Ws), bf16),
            dma((Q, T)),
            dma((Q, J)),
            dma((Q, J)),
            dma((Q, T - 1)),
            dma((Q, T - 1)),
            dma((M,)),
            dma((M, S - 1)),
        ],
        compiler_params=pltpu.CompilerParams(
            collective_id=0, has_side_effects=True, vmem_limit_bytes=60 * 1024 * 1024
        ),
    )(
        coef,
        x0,
        noise,
        temb.reshape(K, 1, W),
        conv_kernel[0],
        norm_gain,
        layer_norm_bias,
        qkv,
        pkv,
        outw,
    )
    ids = jnp.arange(M, dtype=jnp.int32)
    place = jnp.sum(
        jnp.where(entry_order[None, :] == ids[:, None], ids[None, :], 0), axis=1
    )
    return ordered(results, place).reshape(M, rows_here, C, Ws)


def solution(mesh):
    placed = (
        P("batch", "tile", None, None),
        P("batch", None, None),
        P(None, "batch", "tile", None, None),
        P(),
        P("batch"),
        P("section", None, None),
        P("section", None, None),
        P("section", None),
        P("section", None),
        P("section", None, None, "tile"),
        P("section", None, None, "tile"),
        P("section", "tile", None),
    )
    return jax.shard_map(
        per_device,
        mesh=mesh,
        in_specs=placed,
        out_specs=P("batch", "tile", None, "section"),
        check_vma=False,
    )
```

```python
import functools
import math

import jax
import jax.numpy as jnp
from jax import lax
from jax.experimental import pallas as pl
from jax.experimental.pallas import tpu as pltpu
from jax.sharding import PartitionSpec as P

HEADS = 20
LANES = 128
MESH = pl.DeviceIdType.MESH


def noise_plan():
    positions = jnp.arange(1000, dtype=jnp.float32)
    low_root = math.sqrt(0.00085)
    high_root = math.sqrt(0.012)
    roots = low_root + (high_root - low_root) * positions / 999.0
    return jnp.exp(jnp.cumsum(jnp.log(1.0 - roots * roots)))


def time_features(timesteps, half_count):
    exponents = jnp.arange(half_count, dtype=jnp.float32) / half_count
    freq_row = jnp.exp(-math.log(10000.0) * exponents)
    angles = timesteps.astype(jnp.float32)[:, None] * freq_row[None, :]
    return jnp.concatenate([jnp.cos(angles), jnp.sin(angles)], axis=1).astype(jnp.bfloat16)


def chain_kernel(
    dims,
    order_ref,
    steps_ref,
    alpha_ref,
    x0_ref,
    noise_ref,
    temb_ref,
    conv_ref,
    gain_ref,
    bias_ref,
    qkv_ref,
    pkv_ref,
    outw_ref,
    out_ref,
    xin,
    xstart,
    xsend,
    psend,
    precv,
    mixed,
    normed,
    proj,
    osend,
    oland,
    x_recv,
    x_send,
    x_fwd,
    p_recv,
    p_send,
    o_recv,
    o_send,
):
    S, T, G, K, M, C, keys_prompt, local_heads, head_width = dims
    n, W = x0_ref.shape[1], x0_ref.shape[2]
    N = T * n
    Q = K * M
    J = T // G
    P_, CW = xsend.shape[1], xsend.shape[3]
    Hp = outw_ref.shape[0]
    Ws = out_ref.shape[2]
    s = lax.axis_index("section")
    t = lax.axis_index("tile")
    last = s == S - 1
    after = lax.rem(s + 1, S)
    partner = t + 1 - 2 * lax.rem(t, 2)

    barrier = pltpu.get_barrier_semaphore()
    for ds in range(S):
        for dt in range(T):
            if ds or dt:
                pl.semaphore_signal(
                    barrier,
                    inc=1,
                    device_id={"section": lax.rem(s + ds, S), "tile": lax.rem(t + dt, T)},
                    device_id_type=MESH,
                )
    pl.semaphore_wait(barrier, S * T - 1)

    def kin(tile, j):
        return lax.rem(tile + G * j, T)

    def x_copy(src, q, p, j):
        return pltpu.make_async_remote_copy(
            src_ref=src,
            dst_ref=xin.at[q, p, t],
            send_sem=x_send.at[q, p, j],
            recv_sem=x_recv.at[q, p, t],
            device_id={"section": after, "tile": kin(t, j)},
            device_id_type=MESH,
        )

    def x_relay(q, p, j):
        row = kin(t, j)
        return pltpu.make_async_remote_copy(
            src_ref=xin.at[q, p, row],
            dst_ref=xin.at[q, p, row],
            send_sem=x_fwd.at[q, p, j],
            recv_sem=x_recv.at[q, p, row],
            device_id={"section": s, "tile": partner},
            device_id_type=MESH,
        )

    def x_arrived(q, p, row):
        here = xin.at[q, p, row]
        pltpu.make_async_copy(here, here, x_recv.at[q, p, row]).wait()

    def p_copy(q, p, d):
        other = lax.rem(t + d, T)
        return pltpu.make_async_remote_copy(
            src_ref=psend.at[q, p, other],
            dst_ref=precv.at[q, p, d - 1],
            send_sem=p_send.at[q, p, d - 1],
            recv_sem=p_recv.at[q, p, d - 1],
            device_id={"section": s, "tile": other},
            device_id_type=MESH,
        )

    def o_copy(i, d):
        other = lax.rem(s + d, S)
        return pltpu.make_async_remote_copy(
            src_ref=osend.at[i, other],
            dst_ref=oland.at[i],
            send_sem=o_send.at[i, d - 1],
            recv_sem=o_recv.at[i],
            device_id={"section": other, "tile": t},
            device_id_type=MESH,
        )

    @pl.when(last)
    def _():
        for i in range(M):
            row = x0_ref[order_ref[i]]
            for p in range(P_):
                xstart[i, p] = row[:, p * CW : (p + 1) * CW]
            for p in range(P_):
                for j in range(J):
                    x_copy(xstart.at[i, p], i, p, j).start()

    column = lax.rem(lax.broadcasted_iota(jnp.int32, (N, LANES), 0), C)
    at_left = column == 0
    at_right = column == C - 1

    def land(q, p):
        for j in range(J):
            x_arrived(q, p, kin(t, j))
            if G > 1:
                x_relay(q, p, j).start()

    def compute(q, i, level):
        land(q, 0)
        total = jnp.zeros((N, LANES), jnp.float32)
        for p in range(P_):
            if p + 1 < P_:
                land(q, p + 1)
            if G > 1:
                for j in range(J):
                    x_arrived(q, p, kin(partner, j))
            for c in range(CW // LANES):
                sl = slice(p * CW + c * LANES, p * CW + (c + 1) * LANES)
                x = xin[q, p, :, :, c * LANES : (c + 1) * LANES]
                x = x.reshape(N, LANES).astype(jnp.float32)
                x = (x + temb_ref[level, :, sl]).astype(jnp.bfloat16).astype(jnp.float32)
                left = jnp.where(at_left, 0.0, pltpu.roll(x, 1, 0))
                right = jnp.where(at_right, 0.0, pltpu.roll(x, N - 1, 0))
                taps = []
                for a in range(3):
                    taps.append(
                        conv_ref[3 * a : 3 * a + 1, sl] * left
                        + conv_ref[3 * a + 1 : 3 * a + 2, sl] * x
                        + conv_ref[3 * a + 2 : 3 * a + 3, sl] * right
                    )
                edge = jnp.zeros((C, LANES), jnp.float32)
                value = (
                    x
                    + jnp.concatenate([edge, taps[0][: N - C]], axis=0)
                    + taps[1]
                    + jnp.concatenate([taps[2][C:], edge], axis=0)
                )
                mixed[:, :, sl] = value.reshape(T, n, LANES)
                total = total + value
        centre = jnp.sum(total, axis=1, keepdims=True) / W
        total = jnp.zeros((N, LANES), jnp.float32)
        for c in range(W // LANES):
            sl = slice(c * LANES, (c + 1) * LANES)
            delta = mixed[:, :, sl].reshape(N, LANES) - centre
            total = total + delta * delta
        scale = lax.rsqrt(jnp.sum(total, axis=1, keepdims=True) / W + 1e-05)
        for c in range(W // LANES):
            sl = slice(c * LANES, (c + 1) * LANES)
            delta = mixed[:, :, sl].reshape(N, LANES) - centre
            normed[:, sl] = (delta * scale * gain_ref[:, sl] + bias_ref[:, sl]).astype(
                jnp.bfloat16
            )
        proj[...] = jnp.dot(
            normed[...], qkv_ref[...], preferred_element_type=jnp.float32
        ).astype(jnp.bfloat16)
        per_block = LANES // head_width
        latent = order_ref[i]
        blocks = []
        for b in range(Hp // LANES):
            sl = slice(b * LANES, (b + 1) * LANES)
            heads_here = min(per_block, local_heads - b * per_block)
            query = proj[:, sl]
            keys = jnp.concatenate(
                [proj[:, Hp + b * LANES : Hp + (b + 1) * LANES], pkv_ref[latent, 0, :, sl]], axis=0
            )
            values = jnp.concatenate(
                [proj[:, 2 * Hp + b * LANES : 2 * Hp + (b + 1) * LANES], pkv_ref[latent, 1, :, sl]],
                axis=0,
            )
            lane = lax.broadcasted_iota(jnp.int32, (N, LANES), 1) // head_width
            zero = jnp.zeros_like(query)
            stacked = jnp.concatenate(
                [jnp.where(lane == h, query, zero) for h in range(heads_here)], axis=0
            )
            scores = lax.dot_general(
                stacked, keys, (((1,), (1,)), ((), ())), preferred_element_type=jnp.float32
            ) * (1.0 / math.sqrt(head_width))
            real = lax.broadcasted_iota(jnp.int32, scores.shape, 1) < N + keys_prompt
            powers = jnp.where(real, jnp.exp(scores), 0.0)
            soft = (powers * (1.0 / jnp.sum(powers, axis=1, keepdims=True))).astype(jnp.bfloat16)
            got = jnp.dot(soft, values, preferred_element_type=jnp.float32)
            merged = got[:N]
            for h in range(1, heads_here):
                merged = jnp.where(lane == h, got[h * N : (h + 1) * N], merged)
            blocks.append(merged.astype(jnp.bfloat16))
        attended = jnp.concatenate(blocks, axis=1)
        for p in range(P_):
            psend[q, p] = (
                jnp.dot(
                    attended,
                    outw_ref[:, p * CW : (p + 1) * CW],
                    preferred_element_type=jnp.float32,
                )
                .astype(jnp.bfloat16)
                .reshape(T, n, CW)
            )
            for d in range(1, T):
                p_copy(q, p, d).start()

    def finish(q, i, level):
        parts = []
        for p in range(P_):
            for d in range(1, T):
                p_copy(q, p, d).wait_recv()
            update = psend[q, p, t].astype(jnp.float32)
            for d in range(1, T):
                update = update + precv[q, p, d - 1].astype(jnp.float32)
            x = (mixed[t, :, p * CW : (p + 1) * CW] + update).astype(jnp.bfloat16)
            parts.append(x)

            @pl.when(jnp.logical_not(last))
            def _():
                xsend[q, p] = x
                for j in range(J):
                    x_copy(xsend.at[q, p], q, p, j).start()

            if K > 1:

                @pl.when(jnp.logical_and(last, level < K - 1))
                def _():
                    later = lax.rem(level + 1, K)
                    onward = lax.rem(q + M, Q)
                    spot = lax.broadcasted_iota(
                        jnp.int32, alpha_ref.shape, 0
                    ) * LANES + lax.broadcasted_iota(jnp.int32, alpha_ref.shape, 1)
                    alpha = jnp.where(spot == steps_ref[later], alpha_ref[...], 0.0)
                    alpha = jnp.sum(jnp.sum(alpha, axis=1, keepdims=True), axis=0, keepdims=True)
                    fresh = noise_ref[lax.rem(level, K - 1), i, :, p * CW : (p + 1) * CW]
                    xsend[onward, p] = (
                        jnp.sqrt(alpha) * x.astype(jnp.float32)
                        + jnp.sqrt(1.0 - alpha) * fresh.astype(jnp.float32)
                    ).astype(jnp.bfloat16)
                    for j in range(J):
                        x_copy(xsend.at[onward, p], onward, p, j).start()

        @pl.when(jnp.logical_and(last, level == K - 1))
        def _():
            wide = jnp.concatenate(parts, axis=1).astype(jnp.float32)
            for k in range(S):
                turned = wide if k == 0 else pltpu.roll(wide, W - k * Ws, 1)
                piece = turned[:, :Ws].astype(jnp.bfloat16)
                if k < S - 1:
                    osend[i, k] = piece
                else:
                    oland[i] = piece
            for d in range(1, S):
                o_copy(i, d).start()

    def step(q, carry):
        level = q // M
        i = lax.rem(q, M)
        compute(q, i, level)
        finish(q, i, level)
        return carry

    lax.fori_loop(0, Q, step, 0)

    def drain(q, carry):
        for p in range(P_):
            for j in range(J):
                x_copy(xsend.at[q, p], q, p, j).wait_send()
                if G > 1:
                    x_relay(q, p, j).wait_send()
            for d in range(1, T):
                p_copy(q, p, d).wait_send()
        return carry

    lax.fori_loop(0, Q, drain, 0)

    @pl.when(last)
    def _():
        for i in range(M):
            for d in range(1, S):
                o_copy(i, d).wait_send()

    @pl.when(jnp.logical_not(last))
    def _():
        for i in range(M):
            pltpu.make_async_copy(oland.at[i], oland.at[i], o_recv.at[i]).wait()

    for m in range(M):
        entry = 0
        for i in range(M):
            entry = jnp.where(order_ref[i] == m, i, entry)
        out_ref[m] = oland[entry]


def per_device(
    latents,
    prompt_tokens,
    fresh_noise,
    timesteps,
    entry_order,
    timestep_weight,
    conv_kernel,
    norm_gain,
    layer_norm_bias,
    qkv_weight,
    prompt_weight,
    out_weight,
):
    S = lax.axis_size("section")
    T = lax.axis_size("tile")
    M, rows_here, C, W = latents.shape
    n = rows_here * C
    K = timesteps.shape[0]
    Q = K * M
    G = 2 if T % 2 == 0 else 1
    J = T // G
    local_heads = HEADS // T
    head_width = W // HEADS
    H = local_heads * head_width
    Hp = -(-H // LANES) * LANES
    text = prompt_tokens.shape[1]
    text_pad = -(-text // LANES) * LANES
    Ws = W // S
    CW = 2 * LANES if W % (2 * LANES) == 0 else LANES
    pieces = W // CW

    alpha_table = noise_plan()
    alpha_rows = -(-alpha_table.shape[0] // (8 * LANES)) * 8
    alpha_table = jnp.pad(alpha_table, (0, alpha_rows * LANES - alpha_table.shape[0]))
    feature_rows = time_features(timesteps, timestep_weight.shape[1] // 2)
    temb = jnp.dot(feature_rows, timestep_weight[0], preferred_element_type=jnp.float32)

    x0 = latents.reshape(M, n, W)
    noise = fresh_noise.reshape(fresh_noise.shape[0], M, n, W)
    tokens = prompt_tokens.reshape(M * text, prompt_tokens.shape[2])
    pkv = jnp.stack(
        [
            jnp.dot(tokens, prompt_weight[0, :, j], preferred_element_type=jnp.float32)
            .astype(jnp.bfloat16)
            .reshape(M, text, H)
            for j in range(2)
        ],
        axis=1,
    )
    pkv = jnp.pad(pkv, ((0, 0), (0, 0), (0, text_pad - text), (0, Hp - H)))
    qkv = jnp.concatenate(
        [jnp.pad(qkv_weight[0, :, j], ((0, 0), (0, Hp - H))) for j in range(3)], axis=1
    )
    outw = jnp.pad(out_weight[0], ((0, Hp - H), (0, 0)))

    dims = (S, T, G, K, M, C, text, local_heads, head_width)
    vmem = pl.BlockSpec(memory_space=pltpu.VMEM)
    bf16, f32 = jnp.bfloat16, jnp.float32
    dma = pltpu.SemaphoreType.DMA
    results = pl.pallas_call(
        functools.partial(chain_kernel, dims),
        out_shape=jax.ShapeDtypeStruct((M, n, Ws), bf16),
        in_specs=[pl.BlockSpec(memory_space=pltpu.SMEM)] * 2 + [vmem] * 10,
        out_specs=vmem,
        scratch_shapes=[
            pltpu.VMEM((Q, pieces, T, n, CW), bf16),
            pltpu.VMEM((M, pieces, n, CW), bf16),
            pltpu.VMEM((Q, pieces, n, CW), bf16),
            pltpu.VMEM((Q, pieces, T, n, CW), bf16),
            pltpu.VMEM((Q, pieces, T - 1, n, CW), bf16),
            pltpu.VMEM((T, n, W), f32),
            pltpu.VMEM((T * n, W), bf16),
            pltpu.VMEM((T * n, 3 * Hp), bf16),
            pltpu.VMEM((M, S, n, Ws), bf16),
            pltpu.VMEM((M, n, Ws), bf16),
            dma((Q, pieces, T)),
            dma((Q, pieces, J)),
            dma((Q, pieces, J)),
            dma((Q, pieces, T - 1)),
            dma((Q, pieces, T - 1)),
            dma((M,)),
            dma((M, S - 1)),
        ],
        compiler_params=pltpu.CompilerParams(
            collective_id=0, has_side_effects=True, vmem_limit_bytes=60 * 1024 * 1024
        ),
    )(
        entry_order,
        timesteps,
        alpha_table.reshape(alpha_rows, LANES),
        x0,
        noise,
        temb.reshape(K, 1, W),
        conv_kernel[0],
        norm_gain,
        layer_norm_bias,
        qkv,
        pkv,
        outw,
    )
    return results.reshape(M, rows_here, C, Ws)


def solution(mesh):
    placed = (
        P("batch", "tile", None, None),
        P("batch", None, None),
        P(None, "batch", "tile", None, None),
        P(),
        P("batch"),
        P("section", None, None),
        P("section", None, None),
        P("section", None),
        P("section", None),
        P("section", None, None, "tile"),
        P("section", None, None, "tile"),
        P("section", "tile", None),
    )
    return jax.shard_map(
        per_device,
        mesh=mesh,
        in_specs=placed,
        out_specs=P("batch", "tile", None, "section"),
        check_vma=False,
    )
```

```python
import functools
import math

import jax
import jax.numpy as jnp
from jax import lax
from jax.experimental import pallas as pl
from jax.experimental.pallas import tpu as pltpu
from jax.sharding import PartitionSpec as P

HEADS = 20
LANES = 128
MESH = pl.DeviceIdType.MESH


def noise_plan():
    positions = jnp.arange(1000, dtype=jnp.float32)
    low_root = math.sqrt(0.00085)
    high_root = math.sqrt(0.012)
    roots = low_root + (high_root - low_root) * positions / 999.0
    return jnp.exp(jnp.cumsum(jnp.log(1.0 - roots * roots)))


def time_features(timesteps, half_count):
    exponents = jnp.arange(half_count, dtype=jnp.float32) / half_count
    freq_row = jnp.exp(-math.log(10000.0) * exponents)
    angles = timesteps.astype(jnp.float32)[:, None] * freq_row[None, :]
    return jnp.concatenate([jnp.cos(angles), jnp.sin(angles)], axis=1).astype(jnp.bfloat16)


def chain_kernel(
    dims,
    order_ref,
    steps_ref,
    alpha_ref,
    x0_ref,
    noise_ref,
    temb_ref,
    conv_ref,
    gain_ref,
    bias_ref,
    qkv_ref,
    pkv_ref,
    outw_ref,
    out_ref,
    xin,
    xstart,
    xsend,
    psend,
    precv,
    mixed,
    normed,
    proj,
    osend,
    oland,
    x_recv,
    x_send,
    x_fwd,
    p_recv,
    p_send,
    o_recv,
    o_send,
):
    S, T, G, K, M, C, keys_prompt, local_heads, head_width = dims
    n, W = x0_ref.shape[1], x0_ref.shape[2]
    N = T * n
    Q = K * M
    J = T // G
    P_, CW = xsend.shape[1], xsend.shape[3]
    Hp = outw_ref.shape[0]
    Ws = out_ref.shape[2]
    s = lax.axis_index("section")
    t = lax.axis_index("tile")
    last = s == S - 1
    after = lax.rem(s + 1, S)
    partner = t + 1 - 2 * lax.rem(t, 2)

    barrier = pltpu.get_barrier_semaphore()
    for ds in range(S):
        for dt in range(T):
            if ds or dt:
                pl.semaphore_signal(
                    barrier,
                    inc=1,
                    device_id={"section": lax.rem(s + ds, S), "tile": lax.rem(t + dt, T)},
                    device_id_type=MESH,
                )
    pl.semaphore_wait(barrier, S * T - 1)

    def kin(tile, j):
        return lax.rem(tile + G * j, T)

    def x_copy(src, q, p, j):
        return pltpu.make_async_remote_copy(
            src_ref=src,
            dst_ref=xin.at[q, p, t],
            send_sem=x_send.at[q, p, j],
            recv_sem=x_recv.at[q, p, t],
            device_id={"section": after, "tile": kin(t, j)},
            device_id_type=MESH,
        )

    def x_relay(q, p, j):
        row = kin(t, j)
        return pltpu.make_async_remote_copy(
            src_ref=xin.at[q, p, row],
            dst_ref=xin.at[q, p, row],
            send_sem=x_fwd.at[q, p, j],
            recv_sem=x_recv.at[q, p, row],
            device_id={"section": s, "tile": partner},
            device_id_type=MESH,
        )

    def x_arrived(q, p, row):
        here = xin.at[q, p, row]
        pltpu.make_async_copy(here, here, x_recv.at[q, p, row]).wait()

    def p_copy(q, p, d):
        other = lax.rem(t + d, T)
        return pltpu.make_async_remote_copy(
            src_ref=psend.at[q, p, other],
            dst_ref=precv.at[q, p, d - 1],
            send_sem=p_send.at[q, p, d - 1],
            recv_sem=p_recv.at[q, p, d - 1],
            device_id={"section": s, "tile": other},
            device_id_type=MESH,
        )

    def o_copy(i, d):
        other = lax.rem(s + d, S)
        return pltpu.make_async_remote_copy(
            src_ref=osend.at[i, other],
            dst_ref=oland.at[i],
            send_sem=o_send.at[i, d - 1],
            recv_sem=o_recv.at[i],
            device_id={"section": other, "tile": t},
            device_id_type=MESH,
        )

    @pl.when(last)
    def _():
        for i in range(M):
            row = x0_ref[order_ref[i]]
            for p in range(P_):
                xstart[i, p] = row[:, p * CW : (p + 1) * CW]
            for p in range(P_):
                for j in range(J):
                    x_copy(xstart.at[i, p], i, p, j).start()

    column = lax.rem(lax.broadcasted_iota(jnp.int32, (N, LANES), 0), C)
    at_left = column == 0
    at_right = column == C - 1

    def land(q, p):
        for j in range(J):
            x_arrived(q, p, kin(t, j))
            if G > 1:
                x_relay(q, p, j).start()

    def compute(q, i, level):
        land(q, 0)
        total = jnp.zeros((N, LANES), jnp.float32)
        for p in range(P_):
            if p + 1 < P_:
                land(q, p + 1)
            if G > 1:
                for j in range(J):
                    x_arrived(q, p, kin(partner, j))
            for c in range(CW // LANES):
                sl = slice(p * CW + c * LANES, p * CW + (c + 1) * LANES)
                x = xin[q, p, :, :, c * LANES : (c + 1) * LANES]
                x = x.reshape(N, LANES).astype(jnp.float32)
                x = (x + temb_ref[level, :, sl]).astype(jnp.bfloat16).astype(jnp.float32)
                left = jnp.where(at_left, 0.0, pltpu.roll(x, 1, 0))
                right = jnp.where(at_right, 0.0, pltpu.roll(x, N - 1, 0))
                taps = []
                for a in range(3):
                    taps.append(
                        conv_ref[3 * a : 3 * a + 1, sl] * left
                        + conv_ref[3 * a + 1 : 3 * a + 2, sl] * x
                        + conv_ref[3 * a + 2 : 3 * a + 3, sl] * right
                    )
                edge = jnp.zeros((C, LANES), jnp.float32)
                value = (
                    x
                    + jnp.concatenate([edge, taps[0][: N - C]], axis=0)
                    + taps[1]
                    + jnp.concatenate([taps[2][C:], edge], axis=0)
                )
                mixed[:, :, sl] = value.reshape(T, n, LANES)
                total = total + value
        centre = jnp.sum(total, axis=1, keepdims=True) / W
        total = jnp.zeros((N, LANES), jnp.float32)
        for c in range(W // LANES):
            sl = slice(c * LANES, (c + 1) * LANES)
            delta = mixed[:, :, sl].reshape(N, LANES) - centre
            total = total + delta * delta
        scale = lax.rsqrt(jnp.sum(total, axis=1, keepdims=True) / W + 1e-05)
        for c in range(W // LANES):
            sl = slice(c * LANES, (c + 1) * LANES)
            delta = mixed[:, :, sl].reshape(N, LANES) - centre
            normed[:, sl] = (delta * scale * gain_ref[:, sl] + bias_ref[:, sl]).astype(
                jnp.bfloat16
            )
        proj[...] = lax.dot_general(
            normed[...],
            qkv_ref[...],
            (((1,), (1,)), ((), ())),
            preferred_element_type=jnp.float32,
        ).astype(jnp.bfloat16)
        per_block = LANES // head_width
        latent = order_ref[i]
        blocks = []
        for b in range(Hp // LANES):
            sl = slice(b * LANES, (b + 1) * LANES)
            heads_here = min(per_block, local_heads - b * per_block)
            query = proj[:, sl]
            keys = jnp.concatenate(
                [proj[:, Hp + b * LANES : Hp + (b + 1) * LANES], pkv_ref[latent, 0, :, sl]], axis=0
            )
            values = jnp.concatenate(
                [proj[:, 2 * Hp + b * LANES : 2 * Hp + (b + 1) * LANES], pkv_ref[latent, 1, :, sl]],
                axis=0,
            )
            lane = lax.broadcasted_iota(jnp.int32, (N, LANES), 1) // head_width
            zero = jnp.zeros_like(query)
            stacked = jnp.concatenate(
                [jnp.where(lane == h, query, zero) for h in range(heads_here)], axis=0
            )
            scores = lax.dot_general(
                stacked, keys, (((1,), (1,)), ((), ())), preferred_element_type=jnp.float32
            ) * (1.0 / math.sqrt(head_width))
            real = lax.broadcasted_iota(jnp.int32, scores.shape, 1) < N + keys_prompt
            powers = jnp.where(real, jnp.exp(scores), 0.0)
            soft = (powers * (1.0 / jnp.sum(powers, axis=1, keepdims=True))).astype(jnp.bfloat16)
            got = jnp.dot(soft, values, preferred_element_type=jnp.float32)
            merged = got[:N]
            for h in range(1, heads_here):
                merged = jnp.where(lane == h, got[h * N : (h + 1) * N], merged)
            blocks.append(merged.astype(jnp.bfloat16))
        attended = jnp.concatenate(blocks, axis=1)
        for p in range(P_):
            psend[q, p] = (
                jnp.dot(
                    attended,
                    outw_ref[:, p * CW : (p + 1) * CW],
                    preferred_element_type=jnp.float32,
                )
                .astype(jnp.bfloat16)
                .reshape(T, n, CW)
            )
            for d in range(1, T):
                p_copy(q, p, d).start()

    def finish(q, i, level):
        parts = []
        for p in range(P_):
            for d in range(1, T):
                p_copy(q, p, d).wait_recv()
            update = psend[q, p, t].astype(jnp.float32)
            for d in range(1, T):
                update = update + precv[q, p, d - 1].astype(jnp.float32)
            x = (mixed[t, :, p * CW : (p + 1) * CW] + update).astype(jnp.bfloat16)
            parts.append(x)

            @pl.when(jnp.logical_not(last))
            def _():
                xsend[q, p] = x
                for j in range(J):
                    x_copy(xsend.at[q, p], q, p, j).start()

            if K > 1:

                @pl.when(jnp.logical_and(last, level < K - 1))
                def _():
                    later = lax.rem(level + 1, K)
                    onward = lax.rem(q + M, Q)
                    spot = lax.broadcasted_iota(
                        jnp.int32, alpha_ref.shape, 0
                    ) * LANES + lax.broadcasted_iota(jnp.int32, alpha_ref.shape, 1)
                    alpha = jnp.where(spot == steps_ref[later], alpha_ref[...], 0.0)
                    alpha = jnp.sum(jnp.sum(alpha, axis=1, keepdims=True), axis=0, keepdims=True)
                    fresh = noise_ref[lax.rem(level, K - 1), i, :, p * CW : (p + 1) * CW]
                    xsend[onward, p] = (
                        jnp.sqrt(alpha) * x.astype(jnp.float32)
                        + jnp.sqrt(1.0 - alpha) * fresh.astype(jnp.float32)
                    ).astype(jnp.bfloat16)
                    for j in range(J):
                        x_copy(xsend.at[onward, p], onward, p, j).start()

        @pl.when(jnp.logical_and(last, level == K - 1))
        def _():
            wide = jnp.concatenate(parts, axis=1).astype(jnp.float32)
            for k in range(S):
                turned = wide if k == 0 else pltpu.roll(wide, W - k * Ws, 1)
                piece = turned[:, :Ws].astype(jnp.bfloat16)
                if k < S - 1:
                    osend[i, k] = piece
                else:
                    oland[i] = piece
            for d in range(1, S):
                o_copy(i, d).start()

    def step(q, carry):
        level = q // M
        i = lax.rem(q, M)
        compute(q, i, level)
        finish(q, i, level)
        return carry

    lax.fori_loop(0, Q, step, 0)

    def drain(q, carry):
        for p in range(P_):
            for j in range(J):
                x_copy(xsend.at[q, p], q, p, j).wait_send()
                if G > 1:
                    x_relay(q, p, j).wait_send()
            for d in range(1, T):
                p_copy(q, p, d).wait_send()
        return carry

    lax.fori_loop(0, Q, drain, 0)

    @pl.when(last)
    def _():
        for i in range(M):
            for d in range(1, S):
                o_copy(i, d).wait_send()

    @pl.when(jnp.logical_not(last))
    def _():
        for i in range(M):
            pltpu.make_async_copy(oland.at[i], oland.at[i], o_recv.at[i]).wait()

    for m in range(M):
        entry = 0
        for i in range(M):
            entry = jnp.where(order_ref[i] == m, i, entry)
        out_ref[m] = oland[entry]


def per_device(
    latents,
    prompt_tokens,
    fresh_noise,
    timesteps,
    entry_order,
    timestep_weight,
    conv_kernel,
    norm_gain,
    layer_norm_bias,
    qkv_weight,
    prompt_weight,
    out_weight,
):
    S = lax.axis_size("section")
    T = lax.axis_size("tile")
    M, rows_here, C, W = latents.shape
    n = rows_here * C
    K = timesteps.shape[0]
    Q = K * M
    G = 2 if T % 2 == 0 else 1
    J = T // G
    local_heads = HEADS // T
    head_width = W // HEADS
    H = local_heads * head_width
    Hp = -(-H // LANES) * LANES
    text = prompt_tokens.shape[1]
    text_pad = -(-text // LANES) * LANES
    Ws = W // S
    CW = 2 * LANES if W % (2 * LANES) == 0 else LANES
    pieces = W // CW

    alpha_table = noise_plan()
    alpha_rows = -(-alpha_table.shape[0] // (8 * LANES)) * 8
    alpha_table = jnp.pad(alpha_table, (0, alpha_rows * LANES - alpha_table.shape[0]))
    feature_rows = time_features(timesteps, timestep_weight.shape[1] // 2)
    temb = jnp.dot(feature_rows, timestep_weight[0], preferred_element_type=jnp.float32)

    x0 = latents.reshape(M, n, W)
    noise = fresh_noise.reshape(fresh_noise.shape[0], M, n, W)
    tokens = prompt_tokens.reshape(M * text, prompt_tokens.shape[2])
    pkv = jnp.stack(
        [
            jnp.dot(tokens, prompt_weight[0, :, j], preferred_element_type=jnp.float32)
            .astype(jnp.bfloat16)
            .reshape(M, text, H)
            for j in range(2)
        ],
        axis=1,
    )
    pkv = jnp.pad(pkv, ((0, 0), (0, 0), (0, text_pad - text), (0, Hp - H)))
    qkv = jnp.transpose(qkv_weight[0], (1, 2, 0))
    qkv = jnp.pad(qkv, ((0, 0), (0, Hp - H), (0, 0))).reshape(3 * Hp, W)
    outw = jnp.pad(out_weight[0], ((0, Hp - H), (0, 0)))

    dims = (S, T, G, K, M, C, text, local_heads, head_width)
    vmem = pl.BlockSpec(memory_space=pltpu.VMEM)
    bf16, f32 = jnp.bfloat16, jnp.float32
    dma = pltpu.SemaphoreType.DMA
    results = pl.pallas_call(
        functools.partial(chain_kernel, dims),
        out_shape=jax.ShapeDtypeStruct((M, n, Ws), bf16),
        in_specs=[pl.BlockSpec(memory_space=pltpu.SMEM)] * 2 + [vmem] * 10,
        out_specs=vmem,
        scratch_shapes=[
            pltpu.VMEM((Q, pieces, T, n, CW), bf16),
            pltpu.VMEM((M, pieces, n, CW), bf16),
            pltpu.VMEM((Q, pieces, n, CW), bf16),
            pltpu.VMEM((Q, pieces, T, n, CW), bf16),
            pltpu.VMEM((Q, pieces, T - 1, n, CW), bf16),
            pltpu.VMEM((T, n, W), f32),
            pltpu.VMEM((T * n, W), bf16),
            pltpu.VMEM((T * n, 3 * Hp), bf16),
            pltpu.VMEM((M, S, n, Ws), bf16),
            pltpu.VMEM((M, n, Ws), bf16),
            dma((Q, pieces, T)),
            dma((Q, pieces, J)),
            dma((Q, pieces, J)),
            dma((Q, pieces, T - 1)),
            dma((Q, pieces, T - 1)),
            dma((M,)),
            dma((M, S - 1)),
        ],
        compiler_params=pltpu.CompilerParams(
            collective_id=0, has_side_effects=True, vmem_limit_bytes=60 * 1024 * 1024
        ),
    )(
        entry_order,
        timesteps,
        alpha_table.reshape(alpha_rows, LANES),
        x0,
        noise,
        temb.reshape(K, 1, W),
        conv_kernel[0],
        norm_gain,
        layer_norm_bias,
        qkv,
        pkv,
        outw,
    )
    return results.reshape(M, rows_here, C, Ws)


def solution(mesh):
    placed = (
        P("batch", "tile", None, None),
        P("batch", None, None),
        P(None, "batch", "tile", None, None),
        P(),
        P("batch"),
        P("section", None, None),
        P("section", None, None),
        P("section", None),
        P("section", None),
        P("section", None, None, "tile"),
        P("section", None, None, "tile"),
        P("section", "tile", None),
    )
    return jax.shard_map(
        per_device,
        mesh=mesh,
        in_specs=placed,
        out_specs=P("batch", "tile", None, "section"),
        check_vma=False,
    )
```
